32 devices in a mesh: grp: 8 (over z, core), tp: 4 (over y, x).
Axes of the slice: x: 2, y: 2, z: 4, core: 2. Of those that a mesh axis runs over, the one named last changes fastest.
Arguments:
- hidden: bfloat16 [3072, 5120], P('grp'), may hold values from -6 to 6
- merge_weight: bfloat16 [5120, 8192], P(None, 'tp'), may hold values from -0.078125 to 0.078125
- text_embed: bfloat16 [8192, 8192], P('grp', 'tp'), may hold values from -6 to 6
- gain: float32 [8192], P('tp'), may hold values from 0.1 to 1.9
- head_weight: float32 [8192, 19], P('tp'), may hold values from -2 to 2
- owner: int32 [3072, 1], P('grp'), may hold values from 0 to 7; in each aligned block of 384 rows (0 to 383, 384 to 767, ...) at most 96 rows name the same one
- vis_row: int32 [8, 768], P('grp'), may hold values from 0 to 1023, as said below
- lengths: int32 [8], P('grp'), may hold values from 256 to 1024
- labels: int32 [8, 19], replicated, may hold values from 0 to 1, as said below
- targets: float32 [8, 19], P('grp'), may hold values from -4 to 4
Outputs:
- reward: float32 [8, 19], P('grp')
- visual_grad: bfloat16 [3072, 8192], P('grp', 'tp')
- head_grad: float32 [8192, 19], P('tp')
- gain_grad: float32 [8192], P('tp')
The draws below stay inside these ranges and needn't reach their ends.
Inputs may be any that keep to these rules, and one draw needn't show every extreme that they name: `owner`: in each vision group's 384 rows no sample is named more than 96 times, a bound that some block reaches. `vis_row`: each row holds 768 different positions. `labels`: an objective may be rated by no sample.
All inputs are finite; a program needn't handle non-finite values.
Results may differ from the reference program's by a relative error of at most 0.0035.
Values may be sent and summed in bfloat16 or wider, within the bound.
A program may use at most 128 MiB of HBM per device.

```python
import math
import jax
import jax.numpy as jnp
import numpy as np
from jax import lax

D = 8192
HM = 5120
K = 19
M_DEV = 384
S_DEV = 1024
SAMPLES = 8
VIS = 3072
CAP = 96
SLOTS = 768
ROWS = 8192
SCALE = 512
N_GRP = 8


def draw_vis_row(key, part):
    keys = jax.random.split(jax.random.fold_in(key, 17), SAMPLES)

    def one_sample(sample_key):
        return jax.random.permutation(sample_key, S_DEV)[:SLOTS].astype(jnp.int32)
    return jax.vmap(one_sample)(keys)


def draw_labels(key, part):
    base = jax.random.fold_in(key, 29)
    mark_key, order_key, count_key = jax.random.split(base, 3)
    marks = (jax.random.randint(mark_key, (SAMPLES, K), 0, 4) == 0).astype(jnp.int32)
    order = jax.random.permutation(order_key, K).astype(jnp.int32)
    column_rank = jnp.zeros((K,), jnp.int32).at[order].set(jnp.arange(K, dtype=jnp.int32))
    cleared = jax.random.randint(count_key, (), 1, 3).astype(jnp.int32)
    keep = (column_rank >= cleared).astype(jnp.int32)
    return (marks * keep[None, :]).astype(jnp.int32)


def plant(array, stream_key, smallest, high):
    extent = array.shape
    place = [jax.random.randint(jax.random.fold_in(stream_key, axis), (), 0, extent[axis]) for axis in range(len(extent))]
    array = array.at[tuple(place)].set(smallest)
    longest = extent.index(max(extent))
    place[longest] = (place[longest] + 1) % extent[longest]
    return array.at[tuple(place)].set(high)


def levels(rng, dims, cuts, smallest, high):
    level, own = 1.0, jax.random.fold_in(rng, 6)
    for axis_at, shards_of in cuts:
        draws = jnp.exp(jax.random.uniform(jax.random.fold_in(own, axis_at), (shards_of,), jnp.float32, smallest / len(cuts), high / len(cuts)))
        level = level * jnp.repeat(draws, dims[axis_at] // shards_of).reshape([-1 if axis == axis_at else 1 for axis in range(len(dims))])
    return level


def deal_out(key, own, number, rows, amount, top, limit, slope):
    sequence = jax.random.permutation(key, amount)
    crowded, ordinary = shares(amount, rows * top, limit, slope, True), shares(amount, rows * top, limit, slope, False)
    places = jnp.arange(amount)

    def named(tallies, offset_by):
        used = int((tallies > 0).sum())
        fixed = max(1, used // 4)
        moved = fixed + (places - fixed + offset_by * (used - fixed)) % max(1, amount - fixed)
        return jnp.zeros((amount,), jnp.int32).at[sequence[jnp.where(places < fixed, places, moved)]].set(jnp.asarray(tallies, jnp.int32))

    tallies = jnp.where(number % 4 == 0, named(crowded, number // 4), named(ordinary, number - number // 4 - 1))
    mixed = jax.random.permutation(jax.random.fold_in(own, 3), amount)
    source_of, receiver = mixed[0:amount // 2 * 2:2], mixed[1:amount // 2 * 2:2]
    slack = jnp.minimum(tallies[source_of] - 1, limit - tallies[receiver]) // 2
    slack = jnp.where((source_of == sequence[0]) | (receiver == sequence[0]) | (tallies[receiver] == 0), 0, jnp.maximum(slack, 0))
    moved = jax.random.randint(jax.random.fold_in(own, 4), (amount // 2,), 0, 1 << 20) % (slack + 1)
    tallies = tallies.at[source_of].add(-moved).at[receiver].add(moved)
    items = jnp.searchsorted(jnp.cumsum(tallies), jnp.arange(rows * top), side="right").astype(jnp.int32)
    grid = items.reshape(top, rows).T
    grid = grid[jax.random.permutation(jax.random.fold_in(own, 1), rows)]
    offset_by = jax.random.randint(jax.random.fold_in(own, 2), (rows, 1), 0, top)
    return jnp.take_along_axis(grid, (jnp.arange(top)[None, :] + offset_by) % top, axis=1)


def shares(count, total, reach, slope, full):
    loads = [(1 << 20) // math.isqrt(grade ** slope) + 1 for grade in range(1, count + 1)]
    largest = reach if full else min(reach, max(-(-total // count), total * loads[0] // sum(loads)))
    least = 1 if total - largest >= count - 1 else 0
    given, surplus = [largest] + [least] * (count - 1), total - largest - least * (count - 1)
    while surplus > 0:
        movable = [i for i in range(1, count) if given[i] < largest] or [i for i in range(1, count) if given[i] < reach]
        whole, remaining = sum([loads[i] for i in movable]), surplus
        for i in movable:
            extra = min(reach - given[i], max(1, remaining * loads[i] // whole), surplus)
            given[i] = given[i] + extra
            surplus = surplus - extra
    return np.array(given)


def bell_draw(key, extent, spread, most, cuts=(), kind=jnp.bfloat16):
    loudness = levels(key, extent, cuts, -0.22, 0.18) if cuts else 1.0
    values = jax.random.normal(key, extent, jnp.float32) * spread * loudness
    return jnp.minimum(jnp.maximum(values, -most), most).astype(kind)


def setup_inputs(seed: int = 0) -> dict:
    arg_keys = jax.random.split(jax.random.key(seed), 11)
    hidden = bell_draw(arg_keys[0], (VIS, HM), 1.0, 6.0, ((0, 8),))
    merge_weight = bell_draw(arg_keys[1], (HM, D), HM ** -0.5, 0.078125, ((1, 4),))
    text_embed = bell_draw(arg_keys[2], (ROWS, D), 1.0, 6.0, ((0, 8), (1, 4)))
    gain = jnp.clip(1.0 + 0.18 * jax.random.normal(arg_keys[3], (D,), jnp.float32), 0.1, 1.9)
    head_weight = bell_draw(arg_keys[4], (D, K), (D // S_DEV) ** -0.5, 2.0, ((0, 4),), jnp.float32)
    owner_keys = jax.random.split(jax.random.fold_in(arg_keys[5], 1), VIS // M_DEV)
    owner_turns = jax.random.permutation(jax.random.fold_in(arg_keys[5], 3), VIS // M_DEV)
    owner = jax.vmap(lambda own, number: deal_out(jax.random.fold_in(arg_keys[5], 2), own, number, M_DEV, N_GRP, 1, CAP, 2))(owner_keys, owner_turns).reshape((VIS, 1))
    vis_row = draw_vis_row(jax.random.fold_in(arg_keys[10], 71), 0)
    lengths = plant(jax.random.randint(arg_keys[7], (SAMPLES,), S_DEV // 4, S_DEV + 1), jax.random.fold_in(arg_keys[7], 1), S_DEV // 4, S_DEV).astype(jnp.int32)
    labels = draw_labels(jax.random.fold_in(arg_keys[10], 71), 0)
    targets = bell_draw(arg_keys[9], (SAMPLES, K), 1.0, 4.0, ((0, 8),), jnp.float32)
    return {"hidden": hidden, "merge_weight": merge_weight, "text_embed": text_embed, "gain": gain, "head_weight": head_weight, "owner": owner, "vis_row": vis_row, "lengths": lengths, "labels": labels, "targets": targets}


epsilon = 1e-06

def reference(hidden, merge_weight, text_embed, gain, head_weight, owner, vis_row, lengths, labels, targets):
    visual = jnp.dot(hidden, merge_weight, preferred_element_type=jnp.float32).astype(jnp.bfloat16)
    owners = owner[:, 0].reshape(N_GRP, M_DEV).astype(jnp.int32)
    onehot = (owners[:, :, None] == jnp.arange(N_GRP, dtype=jnp.int32)[None, None, :]).astype(jnp.int32)
    slot_rank = (lax.optimization_barrier(jnp.sum(jnp.cumsum(onehot, axis=1) * onehot, axis=2)) - 1).astype(jnp.int32)
    slot_index = (jnp.arange(N_GRP, dtype=jnp.int32)[:, None] * CAP + slot_rank).astype(jnp.int32)
    local_row = vis_row[owners, slot_index].astype(jnp.int32)
    global_row = (owners * S_DEV + local_row).reshape(-1).astype(jnp.int32)
    placed = text_embed.at[global_row].set(visual)
    counts = lax.optimization_barrier(jnp.sum(labels.astype(jnp.float32), axis=0))

    def per_sample(item):
        sample_rows, length, marks, target = item
        xfull = sample_rows.astype(jnp.float32)
        row_sq = lax.optimization_barrier(jnp.sum(xfull * xfull, axis=1))
        inv_rms = lax.rsqrt(row_sq / D + epsilon)
        partial_value = jnp.dot(xfull * gain[None, :], head_weight, precision=lax.Precision.HIGHEST)
        live_rows = (jnp.arange(S_DEV, dtype=jnp.int32) < length).astype(jnp.float32)
        row_weight = live_rows * inv_rms / length.astype(jnp.float32)
        reward = lax.optimization_barrier(jnp.sum(row_weight[:, None] * partial_value, axis=0))
        cotangent = SCALE * marks.astype(jnp.float32) * (reward - target) / jnp.maximum(counts, 1.0)
        head_dir = jnp.dot(head_weight, cotangent, precision=lax.Precision.HIGHEST)
        row_dot = jnp.dot(partial_value, cotangent, precision=lax.Precision.HIGHEST)
        beta_row = row_weight * inv_rms * inv_rms * row_dot / D
        grad_rows = (row_weight[:, None] * (gain * head_dir)[None, :] - beta_row[:, None] * xfull).astype(jnp.bfloat16)
        pooled = lax.optimization_barrier(jnp.sum(row_weight[:, None] * xfull, axis=0))
        return (reward, grad_rows, jnp.outer(gain * pooled, cotangent), pooled * head_dir)
    rewards, grads, head_parts, gain_parts = lax.map(per_sample, (placed.reshape(SAMPLES, S_DEV, D), lengths, labels, targets))
    visual_grad = grads.reshape(-1, D)[global_row]
    return (rewards, visual_grad, lax.optimization_barrier(jnp.sum(head_parts, axis=0)), lax.optimization_barrier(jnp.sum(gain_parts, axis=0)))
```

```python
import functools

import jax
import jax.numpy as jnp
from jax import lax
from jax.experimental import pallas as pl
from jax.experimental.pallas import tpu as pltpu
from jax.sharding import PartitionSpec as P

EPS = 1e-06
CW = 256
F32 = jnp.float32
BF16 = jnp.bfloat16
MESH = pl.DeviceIdType.MESH
HI = lax.Precision.HIGHEST


def iota(shape, dim):
    return lax.broadcasted_iota(jnp.int32, shape, dim)


def dot(a, b, ca, cb, precision=None):
    return lax.dot_general(
        a, b, (((ca,), (cb,)), ((), ())), precision=precision, preferred_element_type=F32
    )


def split2(a):
    hi = a.astype(BF16).astype(F32)
    return hi, a - hi


def split3(a):
    hi, rest = split2(a)
    mid, low = split2(rest)
    return hi, mid, low


def kernel(
    G, T, cap, scale, K, KR,
    hid_hbm, w_hbm, txt_hbm, gain_ref, hwt_ref, own_ref, vis_ref, len_ref, lab_ref, tgt_ref,
    rew_ref, vg_hbm, head_ref, gg_ref,
    hid, wv, tx, xs, og, ghp, gh3, pacc, sqacc, tsq, pk, tsqx, vst, rbuf, zsend, zrecv, zall, ztx,
    in_sem, w_sem, t_sem, o_sem,
    pk_s, pk_r, ts_s, ts_r, vs_s, vs_r, rb_s, rb_r, zs_s, zs_r, za_s, za_r,
):
    M, H = hid.shape
    Fd = tx.shape[1]
    Pn = tx.shape[0]
    SL = vis_ref.shape[1]
    KB = gh3.shape[0] // 3
    N = Fd // CW
    D = Fd * T
    nA = N // 2
    nM = (N - nA) // 2
    nB = N - nA - nM
    RB = Pn // nA
    CB = Fd // nB // 128 * 128
    me = lax.axis_index("grp")
    mt = lax.axis_index("tp")

    pltpu.make_async_copy(hid_hbm, hid, in_sem).start()

    def wcopy(n):
        return pltpu.make_async_copy(
            w_hbm.at[:, pl.ds(pl.multiple_of(n * CW, CW), CW)],
            wv.at[n], w_sem.at[n])

    def tcopy(n):
        rows = pl.ds(pl.multiple_of(n * RB, RB), RB)
        return pltpu.make_async_copy(txt_hbm.at[rows, :], tx.at[rows, :], t_sem.at[n])

    for n in range(N):
        wcopy(n).start()
        if n < nA:
            tcopy(n).start()

    bar = pltpu.get_barrier_semaphore()

    def greet_g(i, c):
        pl.semaphore_signal(bar, inc=1, device_id=(lax.rem(me + i, G), mt), device_id_type=MESH)
        return c

    def greet_t(i, c):
        pl.semaphore_signal(bar, inc=1, device_id=(me, lax.rem(mt + i, T)), device_id_type=MESH)
        return c

    lax.fori_loop(1, G, greet_g, 0)
    lax.fori_loop(1, T, greet_t, 0)

    def grp_copy(src, dst, ss, rs, i):
        peer = lax.rem(me + i, G)
        return pltpu.make_async_remote_copy(
            src, dst, ss.at[i], rs, device_id=(peer, mt), device_id_type=MESH)

    def g_gather(buf, ss, rs, i):
        return grp_copy(buf.at[me], buf.at[me], ss, rs.at[me], i)

    def g_gather_in(buf, ss, rs, i):
        peer = lax.rem(me + i, G)
        return grp_copy(buf.at[peer], buf.at[peer], ss, rs.at[peer], i)

    def t_gather(buf, ss, rs, i, slot):
        return pltpu.make_async_remote_copy(
            buf.at[slot], buf.at[slot], ss.at[i], rs.at[slot],
            device_id=(me, lax.rem(mt + i, T)), device_id_type=MESH)

    def loop(n, f):
        def body(i, c):
            f(i)
            return c
        lax.fori_loop(1, n, body, 0)

    own = own_ref[...]
    oht = (jnp.broadcast_to(own, (G, M)) == iota((G, M), 0)).astype(F32)
    before = (iota((M, M), 0) < iota((M, M), 1)).astype(F32).astype(BF16)
    ohb = oht.astype(BF16)
    rank = jnp.sum(oht * dot(ohb, before, 1, 0), axis=0, keepdims=True)
    counts = dot(jnp.ones((8, M), F32).astype(BF16), ohb, 1, 1)

    length = len_ref[0]
    inv_len = jnp.full((1, 1), 1.0, F32) / jnp.full((1, 1), length, jnp.int32).astype(F32)
    vis = vis_ref[...]
    live = jnp.where(vis < length, jnp.broadcast_to(inv_len, vis.shape), 0.0)
    pk[me] = jnp.zeros(pk.shape[1:], F32)
    pk[me, 0:1, :] = live
    pk[me, 1:2, 0:G] = counts[0:1, :]
    pk[me, 2:3, 0:K] = tgt_ref[...]
    pl.semaphore_wait(bar, G - 1 + T - 1)
    loop(G, lambda i: g_gather(pk, pk_s, pk_r, i).start())

    ghp[...] = jnp.zeros(ghp.shape, F32)
    ghp[0:K, :] = hwt_ref[...] * gain_ref[...]
    hi, mid, low = split3(ghp[...])
    gh3[0:KB, :] = hi.astype(BF16)
    gh3[KB:2 * KB, :] = mid.astype(BF16)
    gh3[2 * KB:3 * KB, :] = low.astype(BF16)
    pacc[...] = jnp.zeros(pacc.shape, F32)
    sqacc[...] = jnp.zeros(sqacc.shape, F32)
    pltpu.make_async_copy(hid_hbm, hid, in_sem).wait()

    def project(n):
        wcopy(n).wait()
        cols = pl.ds(pl.multiple_of(n * CW, CW), CW)
        x = jnp.dot(hid[...], wv[n], preferred_element_type=F32).astype(BF16)
        xs[:, cols] = x
        pacc[...] += dot(gh3[:, cols], x, 1, 1)
        xf = x.astype(F32)
        sq = xf * xf
        sqacc[...] += functools.reduce(
            lambda a, b: a + b, [sq[:, c:c + 128] for c in range(0, CW, 128)])

    def phase_a(n, c):
        project(n)
        tcopy(n).wait()
        rows = pl.ds(pl.multiple_of(n * RB, RB), RB)
        acc = None
        for t in range(0, Fd, 128):
            xf = tx[rows, t:t + 128].astype(F32)
            acc = xf * xf if acc is None else acc + xf * xf
        tsq[rows, :] = acc
        return c

    lax.fori_loop(0, nA, phase_a, 0)
    tsum = jnp.sum(tsq[...].T, axis=0, keepdims=True)
    tsqx[mt] = jnp.broadcast_to(tsum, (8, Pn))
    loop(T, lambda i: t_gather(tsqx, ts_s, ts_r, i, mt).start())

    def phase_m(n, c):
        project(n)
        return c

    lax.fori_loop(nA, nA + nM, phase_m, 0)

    loop(G, lambda i: g_gather_in(pk, pk_s, pk_r, i).wait_recv())
    loop(T, lambda i: t_gather(tsqx, ts_s, ts_r, i, lax.rem(mt + i, T)).wait_recv())
    cnt_of = jnp.sum(
        jnp.where(iota((G, 128), 1) == me, pk[:, 1, 0:128], 0.0), axis=1, keepdims=True)
    slot = iota((G, SL), 1) - iota((G, SL), 0) * cap
    held = jnp.max(
        jnp.where((slot >= 0) & (slot < cnt_of.astype(jnp.int32)), 1.0, 0.0),
        axis=0, keepdims=True)
    visf = jnp.where(held > 0, vis.astype(F32), -1.0)
    vist = jnp.broadcast_to(visf, (128, SL)).T
    dead = []
    for b in range(0, Pn, 128):
        pos = (iota((SL, 128), 1) + b).astype(F32)
        dead.append(jnp.max(jnp.where(vist == pos, 1.0, 0.0), axis=0, keepdims=True))
    dead = jnp.concatenate(dead, axis=1)
    tot = tsqx[0][0:1, :]
    for i in range(1, T):
        tot = tot + tsqx[i][0:1, :]
    tw = jnp.where(
        (iota((1, Pn), 1) < length) & (dead == 0), lax.rsqrt(tot / D + EPS) * inv_len, 0.0)
    th, tm, tl = split3(jnp.broadcast_to(tw, (8, Pn)))
    row8 = iota((8, Pn), 0)
    tw3 = jnp.where(
        row8 == 0, th, jnp.where(row8 == 1, tm, jnp.where(row8 == 2, tl, 0.0))).astype(BF16)

    def phase_b(n, c):
        project(n)
        cols = pl.ds(pl.multiple_of((n - nA - nM) * CB, 128), CB)
        z3 = jnp.dot(tw3, tx[:, cols], preferred_element_type=F32)
        ztx[:, cols] = jnp.broadcast_to(jnp.sum(z3, axis=0, keepdims=True), (8, CB))
        return c

    lax.fori_loop(nA + nM, N, phase_b, 0)
    trew = dot(ztx[...], ghp[...], 1, 1, HI)

    sq = jnp.sum(sqacc[...].T, axis=0, keepdims=True)
    pt = pacc[0:KB, :] + pacc[KB:2 * KB, :] + pacc[2 * KB:3 * KB, :]
    vst[mt] = jnp.zeros(vst.shape[1:], F32)
    vst[mt, 0:KR, :] = pt[0:KR, :]
    vst[mt, K:K + 1, :] = sq
    vst[mt, KR:KR + 8, 0:KB] = trew
    loop(T, lambda i: t_gather(vst, vs_s, vs_r, i, mt).start())

    lg = pk[:, 0, :]
    sel = dot(lg, oht, 0, 0, HI)
    at = rank.astype(jnp.int32) + me * cap
    ltok = jnp.sum(jnp.where(iota((SL, M), 0) == at, sel, 0.0), axis=0, keepdims=True)
    loop(T, lambda i: t_gather(vst, vs_s, vs_r, i, lax.rem(mt + i, T)).wait_recv())
    st = vst[0]
    for i in range(1, T):
        st = st + vst[i]
    ptot = st[0:KR, :]
    inv = lax.rsqrt(st[K:K + 1, :] / D + EPS)
    w = inv * ltok
    wt = oht * w
    rpart = dot(wt, ptot, 1, 1, HI)
    mine = iota((G, KR), 0) == me
    rbuf[me] = jnp.zeros(rbuf.shape[1:], F32)
    rbuf[me, :, 0:KR] = rpart + jnp.where(mine, st[KR:KR + 1, 0:KR], 0.0)
    loop(G, lambda i: g_gather(rbuf, rb_s, rb_r, i).start())

    wh, wm, wl = split3(wt)
    w3 = jnp.concatenate([wh, wm, wl], axis=0).astype(BF16)
    z3 = jnp.dot(w3, xs[...], preferred_element_type=F32)
    z = z3[0:G] + z3[G:2 * G] + z3[2 * G:3 * G]
    z = z + jnp.where(iota((G, Fd), 0) == me, ztx[0:1, :], 0.0)
    for t in range(Fd // 128):
        zsend[:, t, :] = z[:, t * 128:(t + 1) * 128]

    def zscatter(i):
        peer = lax.rem(me + i, G)
        return grp_copy(zsend.at[peer], zrecv.at[me], zs_s, zs_r.at[me], i)

    def zscatter_in(i):
        peer = lax.rem(me + i, G)
        return grp_copy(zsend.at[peer], zrecv.at[peer], zs_s, zs_r.at[peer], i)

    loop(G, lambda i: zscatter(i).start())
    zrecv[me] = zsend[me]

    loop(G, lambda i: g_gather_in(rbuf, rb_s, rb_r, i).wait_recv())
    rew = rbuf[0]
    for i in range(1, G):
        rew = rew + rbuf[i]
    rew = rew[:, 0:K]
    rew_ref[...] = jnp.sum(
        jnp.where(iota((G, K), 0) == me, rew, 0.0), axis=0, keepdims=True)
    marks = lab_ref[...].astype(F32)
    total = jnp.maximum(jnp.sum(marks, axis=0, keepdims=True), 1.0)
    cot = scale * marks * (rew - pk[:, 2, 0:K]) / total
    v = dot(cot, hwt_ref[...], 1, 0, HI)
    arow = jnp.sum(ptot[0:K, :] * dot(cot, oht, 0, 0, HI), axis=0, keepdims=True)
    beta = w * inv * inv * arow / D
    bcol = jnp.broadcast_to(beta, (128, M)).T

    loop(G, lambda i: zscatter_in(i).wait_recv())
    zs = zrecv[0]
    for i in range(1, G):
        zs = zs + zrecv[i]
    zall[me] = zs
    loop(G, lambda i: g_gather(zall, za_s, za_r, i).start())

    gv = gain_ref[...] * v
    gh, gl = split2(gv)
    lhs = jnp.concatenate([wh, wm, wh], axis=0).astype(BF16)
    og_rhs = jnp.concatenate([gh, gh, gl], axis=0).astype(BF16)
    bfull = jnp.concatenate([bcol] * (CW // 128), axis=1)

    def ocopy(n):
        cols = slice(n * CW, (n + 1) * CW)
        return pltpu.make_async_copy(og.at[:, cols], vg_hbm.at[:, cols], o_sem.at[n])

    for n in range(N):
        cols = slice(n * CW, (n + 1) * CW)
        part = dot(lhs, og_rhs[:, cols], 0, 0)
        og[:, cols] = (part - bfull * xs[:, cols].astype(F32)).astype(BF16)
        ocopy(n).start()

    loop(G, lambda i: g_gather_in(zall, za_s, za_r, i).wait_recv())
    zf = jnp.concatenate([zall[:, t, :] for t in range(Fd // 128)], axis=1)
    head_ref[...] = gain_ref[...] * dot(cot, zf, 0, 0, HI)
    gg_ref[...] = jnp.sum(zf * v, axis=0, keepdims=True)

    for n in range(N):
        ocopy(n).wait()
    loop(G, lambda i: g_gather(pk, pk_s, pk_r, i).wait_send())
    loop(T, lambda i: t_gather(tsqx, ts_s, ts_r, i, mt).wait_send())
    loop(T, lambda i: t_gather(vst, vs_s, vs_r, i, mt).wait_send())
    loop(G, lambda i: g_gather(rbuf, rb_s, rb_r, i).wait_send())
    loop(G, lambda i: zscatter(i).wait_send())
    loop(G, lambda i: g_gather(zall, za_s, za_r, i).wait_send())


def on_device(
    hidden, merge_weight, text_embed, gain, head_weight, owner, vis_row, lengths, labels, targets
):
    G = lax.axis_size("grp")
    T = lax.axis_size("tp")
    M, H = hidden.shape
    cap = 2 * M // G
    Pn, Fd = text_embed.shape
    K = head_weight.shape[1]
    SL = vis_row.shape[1]
    KR = (K + 1 + 7) // 8 * 8
    KB = (KR + 15) // 16 * 16
    N = Fd // CW
    nA = N // 2
    scale = float(Pn * G // 16)
    vmem = pl.BlockSpec(memory_space=pltpu.VMEM)
    hbm = pl.BlockSpec(memory_space=pl.ANY)
    dma = pltpu.SemaphoreType.DMA
    reward, grad, head, gg = pl.pallas_call(
        functools.partial(kernel, G, T, cap, scale, K, KR),
        name="relay",
        out_shape=(
            jax.ShapeDtypeStruct((1, K), F32),
            jax.ShapeDtypeStruct((M, Fd), BF16),
            jax.ShapeDtypeStruct((K, Fd), F32),
            jax.ShapeDtypeStruct((1, Fd), F32),
        ),
        in_specs=[hbm, hbm, hbm, vmem, vmem, vmem, vmem,
                  pl.BlockSpec(memory_space=pltpu.SMEM), vmem, vmem],
        out_specs=(vmem, hbm, vmem, vmem),
        scratch_shapes=[
            pltpu.VMEM((M, H), BF16),
            pltpu.VMEM((N, H, CW), BF16),
            pltpu.VMEM((Pn, Fd), BF16),
            pltpu.VMEM((M, Fd), BF16),
            pltpu.VMEM((M, Fd), BF16),
            pltpu.VMEM((KB, Fd), F32),
            pltpu.VMEM((3 * KB, Fd), BF16),
            pltpu.VMEM((3 * KB, M), F32),
            pltpu.VMEM((M, 128), F32),
            pltpu.VMEM((Pn, 128), F32),
            pltpu.VMEM((G, 8, SL), F32),
            pltpu.VMEM((T, 8, Pn), F32),
            pltpu.VMEM((T, KR + 8, M), F32),
            pltpu.VMEM((G, G, 128), F32),
            pltpu.VMEM((G, Fd // 128, 128), F32),
            pltpu.VMEM((G, Fd // 128, 128), F32),
            pltpu.VMEM((G, Fd // 128, 128), F32),
            pltpu.VMEM((8, Fd), F32),
            dma, dma((N,)), dma((nA,)), dma((N,)),
            dma((G,)), dma((G,)), dma((T,)), dma((T,)), dma((T,)), dma((T,)),
            dma((G,)), dma((G,)), dma((G,)), dma((G,)), dma((G,)), dma((G,)),
        ],
        compiler_params=pltpu.CompilerParams(
            collective_id=0, has_side_effects=True, vmem_limit_bytes=60 * 1024 * 1024),
    )(hidden, merge_weight, text_embed, gain[None, :], head_weight.T, owner.T,
      vis_row, lengths, labels, targets)
    return reward, grad, head.T, gg[0]


def solution(mesh):
    placed = (
        P("grp", None),
        P(None, "tp"),
        P("grp", "tp"),
        P("tp"),
        P("tp", None),
        P("grp", None),
        P("grp", None),
        P("grp"),
        P(),
        P("grp", None),
    )
    return jax.shard_map(
        on_device,
        mesh=mesh,
        in_specs=placed,
        out_specs=(P("grp", None), P("grp", "tp"), P("tp", None), P("tp")),
        check_vma=False,
    )
```

```python
import functools

import jax
import jax.numpy as jnp
from jax import lax
from jax.experimental import pallas as pl
from jax.experimental.pallas import tpu as pltpu
from jax.sharding import PartitionSpec as P

EPS = 1e-06
CW = 256
F32 = jnp.float32
BF16 = jnp.bfloat16
MESH = pl.DeviceIdType.MESH
HI = lax.Precision.HIGHEST


def iota(shape, dim):
    return lax.broadcasted_iota(jnp.int32, shape, dim)


def dot(a, b, ca, cb, precision=None):
    return lax.dot_general(
        a, b, (((ca,), (cb,)), ((), ())), precision=precision, preferred_element_type=F32
    )


def split2(a):
    hi = a.astype(BF16).astype(F32)
    return hi, a - hi


def split3(a):
    hi, rest = split2(a)
    mid, low = split2(rest)
    return hi, mid, low


def kernel(
    G, T, cap, scale, K, KR,
    hid_hbm, w_hbm, txt_hbm, gain_ref, hwt_ref, own_ref, vis_ref, len_ref, lab_ref, tgt_ref,
    rew_ref, x_hbm, head_ref, gg_ref, lhs_ref, rhs_ref, bcol_ref,
    hid, wv, tx, xs, ghp, gh3, pacc, sqacc, tsq, pk, tsqx, vst, rbuf, zsend, zrecv, zall, ztx,
    in_sem, w_sem, t_sem, o_sem,
    pk_s, pk_r, ts_s, ts_r, vs_s, vs_r, rb_s, rb_r, zs_s, zs_r, za_s, za_r,
):
    M, H = hid.shape
    Fd = tx.shape[1]
    Pn = tx.shape[0]
    SL = vis_ref.shape[1]
    KB = gh3.shape[0] // 3
    N = Fd // CW
    D = Fd * T
    nA = N // 2
    nM = (N - nA) // 2
    nB = N - nA - nM
    RB = Pn // nA
    CB = Fd // nB // 128 * 128
    me = lax.axis_index("grp")
    mt = lax.axis_index("tp")

    pltpu.make_async_copy(hid_hbm, hid, in_sem).start()

    def wcopy(n):
        return pltpu.make_async_copy(
            w_hbm.at[:, pl.ds(pl.multiple_of(n * CW, CW), CW)],
            wv.at[n], w_sem.at[n])

    def tcopy(n):
        rows = pl.ds(pl.multiple_of(n * RB, RB), RB)
        return pltpu.make_async_copy(txt_hbm.at[rows, :], tx.at[rows, :], t_sem.at[n])

    for n in range(N):
        wcopy(n).start()
        if n < nA:
            tcopy(n).start()

    bar = pltpu.get_barrier_semaphore()

    def greet_g(i, c):
        pl.semaphore_signal(bar, inc=1, device_id=(lax.rem(me + i, G), mt), device_id_type=MESH)
        return c

    def greet_t(i, c):
        pl.semaphore_signal(bar, inc=1, device_id=(me, lax.rem(mt + i, T)), device_id_type=MESH)
        return c

    lax.fori_loop(1, G, greet_g, 0)
    lax.fori_loop(1, T, greet_t, 0)

    def grp_copy(src, dst, ss, rs, i):
        peer = lax.rem(me + i, G)
        return pltpu.make_async_remote_copy(
            src, dst, ss.at[i], rs, device_id=(peer, mt), device_id_type=MESH)

    def g_gather(buf, ss, rs, i):
        return grp_copy(buf.at[me], buf.at[me], ss, rs.at[me], i)

    def g_gather_in(buf, ss, rs, i):
        peer = lax.rem(me + i, G)
        return grp_copy(buf.at[peer], buf.at[peer], ss, rs.at[peer], i)

    def t_gather(buf, ss, rs, i, slot):
        return pltpu.make_async_remote_copy(
            buf.at[slot], buf.at[slot], ss.at[i], rs.at[slot],
            device_id=(me, lax.rem(mt + i, T)), device_id_type=MESH)

    def loop(n, f):
        def body(i, c):
            f(i)
            return c
        lax.fori_loop(1, n, body, 0)

    own = own_ref[...]
    oht = (jnp.broadcast_to(own, (G, M)) == iota((G, M), 0)).astype(F32)
    before = (iota((M, M), 0) < iota((M, M), 1)).astype(F32).astype(BF16)
    ohb = oht.astype(BF16)
    rank = jnp.sum(oht * dot(ohb, before, 1, 0), axis=0, keepdims=True)
    counts = dot(jnp.ones((8, M), F32).astype(BF16), ohb, 1, 1)

    length = len_ref[0]
    inv_len = jnp.full((1, 1), 1.0, F32) / jnp.full((1, 1), length, jnp.int32).astype(F32)
    vis = vis_ref[...]
    live = jnp.where(vis < length, jnp.broadcast_to(inv_len, vis.shape), 0.0)
    pk[me] = jnp.zeros(pk.shape[1:], F32)
    pk[me, 0:1, :] = live
    pk[me, 1:2, 0:G] = counts[0:1, :]
    pk[me, 2:3, 0:K] = tgt_ref[...]
    pl.semaphore_wait(bar, G - 1 + T - 1)
    loop(G, lambda i: g_gather(pk, pk_s, pk_r, i).start())

    ghp[...] = jnp.zeros(ghp.shape, F32)
    ghp[0:K, :] = hwt_ref[...] * gain_ref[...]
    hi, mid, low = split3(ghp[...])
    gh3[0:KB, :] = hi.astype(BF16)
    gh3[KB:2 * KB, :] = mid.astype(BF16)
    gh3[2 * KB:3 * KB, :] = low.astype(BF16)
    pacc[...] = jnp.zeros(pacc.shape, F32)
    sqacc[...] = jnp.zeros(sqacc.shape, F32)
    pltpu.make_async_copy(hid_hbm, hid, in_sem).wait()

    def xcopy(n):
        cols = pl.ds(pl.multiple_of(n * CW, CW), CW)
        return pltpu.make_async_copy(xs.at[:, cols], x_hbm.at[:, cols], o_sem.at[n])

    def project(n):
        wcopy(n).wait()
        cols = pl.ds(pl.multiple_of(n * CW, CW), CW)
        x = jnp.dot(hid[...], wv[n], preferred_element_type=F32).astype(BF16)
        xs[:, cols] = x
        xcopy(n).start()
        pacc[...] += dot(gh3[:, cols], x, 1, 1)
        xf = x.astype(F32)
        sq = xf * xf
        sqacc[...] += functools.reduce(
            lambda a, b: a + b, [sq[:, c:c + 128] for c in range(0, CW, 128)])

    def phase_a(n, c):
        project(n)
        tcopy(n).wait()
        rows = pl.ds(pl.multiple_of(n * RB, RB), RB)
        acc = None
        for t in range(0, Fd, 128):
            xf = tx[rows, t:t + 128].astype(F32)
            acc = xf * xf if acc is None else acc + xf * xf
        tsq[rows, :] = acc
        return c

    lax.fori_loop(0, nA, phase_a, 0)
    tsum = jnp.sum(tsq[...].T, axis=0, keepdims=True)
    tsqx[mt] = jnp.broadcast_to(tsum, (8, Pn))
    loop(T, lambda i: t_gather(tsqx, ts_s, ts_r, i, mt).start())

    def phase_m(n, c):
        project(n)
        return c

    lax.fori_loop(nA, nA + nM, phase_m, 0)

    loop(G, lambda i: g_gather_in(pk, pk_s, pk_r, i).wait_recv())
    loop(T, lambda i: t_gather(tsqx, ts_s, ts_r, i, lax.rem(mt + i, T)).wait_recv())
    cnt_of = jnp.sum(
        jnp.where(iota((G, 128), 1) == me, pk[:, 1, 0:128], 0.0), axis=1, keepdims=True)
    slot = iota((G, SL), 1) - iota((G, SL), 0) * cap
    held = jnp.max(
        jnp.where((slot >= 0) & (slot < cnt_of.astype(jnp.int32)), 1.0, 0.0),
        axis=0, keepdims=True)
    visf = jnp.where(held > 0, vis.astype(F32), -1.0)
    vist = jnp.broadcast_to(visf, (128, SL)).T
    dead = []
    for b in range(0, Pn, 128):
        pos = (iota((SL, 128), 1) + b).astype(F32)
        dead.append(jnp.max(jnp.where(vist == pos, 1.0, 0.0), axis=0, keepdims=True))
    dead = jnp.concatenate(dead, axis=1)
    tot = tsqx[0][0:1, :]
    for i in range(1, T):
        tot = tot + tsqx[i][0:1, :]
    tw = jnp.where(
        (iota((1, Pn), 1) < length) & (dead == 0), lax.rsqrt(tot / D + EPS) * inv_len, 0.0)
    th, tm, tl = split3(jnp.broadcast_to(tw, (8, Pn)))
    row8 = iota((8, Pn), 0)
    tw3 = jnp.where(
        row8 == 0, th, jnp.where(row8 == 1, tm, jnp.where(row8 == 2, tl, 0.0))).astype(BF16)

    def phase_b(n, c):
        project(n)
        cols = pl.ds(pl.multiple_of((n - nA - nM) * CB, 128), CB)
        z3 = jnp.dot(tw3, tx[:, cols], preferred_element_type=F32)
        ztx[:, cols] = jnp.broadcast_to(jnp.sum(z3, axis=0, keepdims=True), (8, CB))
        return c

    lax.fori_loop(nA + nM, N, phase_b, 0)
    trew = dot(ztx[...], ghp[...], 1, 1, HI)

    sq = jnp.sum(sqacc[...].T, axis=0, keepdims=True)
    pt = pacc[0:KB, :] + pacc[KB:2 * KB, :] + pacc[2 * KB:3 * KB, :]
    vst[mt] = jnp.zeros(vst.shape[1:], F32)
    vst[mt, 0:KR, :] = pt[0:KR, :]
    vst[mt, K:K + 1, :] = sq
    vst[mt, KR:KR + 8, 0:KB] = trew
    loop(T, lambda i: t_gather(vst, vs_s, vs_r, i, mt).start())

    lg = pk[:, 0, :]
    sel = dot(lg, oht, 0, 0, HI)
    at = rank.astype(jnp.int32) + me * cap
    ltok = jnp.sum(jnp.where(iota((SL, M), 0) == at, sel, 0.0), axis=0, keepdims=True)
    loop(T, lambda i: t_gather(vst, vs_s, vs_r, i, lax.rem(mt + i, T)).wait_recv())
    st = vst[0]
    for i in range(1, T):
        st = st + vst[i]
    ptot = st[0:KR, :]
    inv = lax.rsqrt(st[K:K + 1, :] / D + EPS)
    w = inv * ltok
    wt = oht * w
    rpart = dot(wt, ptot, 1, 1, HI)
    mine = iota((G, KR), 0) == me
    rbuf[me] = jnp.zeros(rbuf.shape[1:], F32)
    rbuf[me, :, 0:KR] = rpart + jnp.where(mine, st[KR:KR + 1, 0:KR], 0.0)
    loop(G, lambda i: g_gather(rbuf, rb_s, rb_r, i).start())

    wh, wm, wl = split3(wt)
    w3 = jnp.concatenate([wh, wm, wl], axis=0).astype(BF16)
    z3 = jnp.dot(w3, xs[...], preferred_element_type=F32)
    z = z3[0:G] + z3[G:2 * G] + z3[2 * G:3 * G]
    z = z + jnp.where(iota((G, Fd), 0) == me, ztx[0:1, :], 0.0)
    for t in range(Fd // 128):
        zsend[:, t, :] = z[:, t * 128:(t + 1) * 128]

    def zscatter(i):
        peer = lax.rem(me + i, G)
        return grp_copy(zsend.at[peer], zrecv.at[me], zs_s, zs_r.at[me], i)

    def zscatter_in(i):
        peer = lax.rem(me + i, G)
        return grp_copy(zsend.at[peer], zrecv.at[peer], zs_s, zs_r.at[peer], i)

    loop(G, lambda i: zscatter(i).start())
    zrecv[me] = zsend[me]

    loop(G, lambda i: g_gather_in(rbuf, rb_s, rb_r, i).wait_recv())
    rew = rbuf[0]
    for i in range(1, G):
        rew = rew + rbuf[i]
    rew = rew[:, 0:K]
    rew_ref[...] = jnp.sum(
        jnp.where(iota((G, K), 0) == me, rew, 0.0), axis=0, keepdims=True)
    marks = lab_ref[...].astype(F32)
    total = jnp.maximum(jnp.sum(marks, axis=0, keepdims=True), 1.0)
    cot = scale * marks * (rew - pk[:, 2, 0:K]) / total
    v = dot(cot, hwt_ref[...], 1, 0, HI)
    arow = jnp.sum(ptot[0:K, :] * dot(cot, oht, 0, 0, HI), axis=0, keepdims=True)
    beta = w * inv * inv * arow / D
    bcol = jnp.broadcast_to(beta, (128, M)).T

    loop(G, lambda i: zscatter_in(i).wait_recv())
    zs = zrecv[0]
    for i in range(1, G):
        zs = zs + zrecv[i]
    zall[me] = zs
    loop(G, lambda i: g_gather(zall, za_s, za_r, i).start())

    gv = gain_ref[...] * v
    gh, gl = split2(gv)
    lhs_ref[...] = jnp.concatenate([wh, wm, wh], axis=0).astype(BF16)
    rhs_ref[...] = jnp.concatenate([gh, gh, gl], axis=0).astype(BF16)
    bcol_ref[...] = bcol

    loop(G, lambda i: g_gather_in(zall, za_s, za_r, i).wait_recv())
    zf = jnp.concatenate([zall[:, t, :] for t in range(Fd // 128)], axis=1)
    head_ref[...] = gain_ref[...] * dot(cot, zf, 0, 0, HI)
    gg_ref[...] = jnp.sum(zf * v, axis=0, keepdims=True)

    for n in range(N):
        xcopy(n).wait()
    loop(G, lambda i: g_gather(pk, pk_s, pk_r, i).wait_send())
    loop(T, lambda i: t_gather(tsqx, ts_s, ts_r, i, mt).wait_send())
    loop(T, lambda i: t_gather(vst, vs_s, vs_r, i, mt).wait_send())
    loop(G, lambda i: g_gather(rbuf, rb_s, rb_r, i).wait_send())
    loop(G, lambda i: zscatter(i).wait_send())
    loop(G, lambda i: g_gather(zall, za_s, za_r, i).wait_send())


def finish(
    x_hbm, lhs_ref, rhs_ref, bcol_ref, rew_in, head_in, gg_in, rew_ref, vg_hbm, head_ref, gg_ref,
    xv, og, i_sem, o_sem,
):
    N = xv.shape[1] // CW

    def move(src, dst, sem, n):
        cols = slice(n * CW, (n + 1) * CW)
        return pltpu.make_async_copy(src.at[:, cols], dst.at[:, cols], sem.at[n])

    for n in range(N):
        move(x_hbm, xv, i_sem, n).start()
    rew_ref[...] = rew_in[...]
    head_ref[...] = head_in[...]
    gg_ref[...] = gg_in[...]
    bfull = jnp.concatenate([bcol_ref[...]] * (CW // 128), axis=1)
    for n in range(N):
        cols = slice(n * CW, (n + 1) * CW)
        part = dot(lhs_ref[...], rhs_ref[:, cols], 0, 0)
        move(x_hbm, xv, i_sem, n).wait()
        og[:, cols] = (part - bfull * xv[:, cols].astype(F32)).astype(BF16)
        move(og, vg_hbm, o_sem, n).start()
    for n in range(N):
        move(og, vg_hbm, o_sem, n).wait()


def on_device(
    hidden, merge_weight, text_embed, gain, head_weight, owner, vis_row, lengths, labels, targets
):
    G = lax.axis_size("grp")
    T = lax.axis_size("tp")
    M, H = hidden.shape
    cap = 2 * M // G
    Pn, Fd = text_embed.shape
    K = head_weight.shape[1]
    SL = vis_row.shape[1]
    KR = (K + 1 + 7) // 8 * 8
    KB = (KR + 15) // 16 * 16
    N = Fd // CW
    nA = N // 2
    scale = float(Pn * G // 16)
    vmem = pl.BlockSpec(memory_space=pltpu.VMEM)
    hbm = pl.BlockSpec(memory_space=pl.ANY)
    dma = pltpu.SemaphoreType.DMA
    reward, x, head, gg, lhs, rhs, bcol = pl.pallas_call(
        functools.partial(kernel, G, T, cap, scale, K, KR),
        name="relay",
        out_shape=(
            jax.ShapeDtypeStruct((1, K), F32),
            jax.ShapeDtypeStruct((M, Fd), BF16),
            jax.ShapeDtypeStruct((K, Fd), F32),
            jax.ShapeDtypeStruct((1, Fd), F32),
            jax.ShapeDtypeStruct((3 * G, M), BF16),
            jax.ShapeDtypeStruct((3 * G, Fd), BF16),
            jax.ShapeDtypeStruct((M, 128), F32),
        ),
        in_specs=[hbm, hbm, hbm, vmem, vmem, vmem, vmem,
                  pl.BlockSpec(memory_space=pltpu.SMEM), vmem, vmem],
        out_specs=(vmem, hbm, vmem, vmem, vmem, vmem, vmem),
        scratch_shapes=[
            pltpu.VMEM((M, H), BF16),
            pltpu.VMEM((N, H, CW), BF16),
            pltpu.VMEM((Pn, Fd), BF16),
            pltpu.VMEM((M, Fd), BF16),
            pltpu.VMEM((KB, Fd), F32),
            pltpu.VMEM((3 * KB, Fd), BF16),
            pltpu.VMEM((3 * KB, M), F32),
            pltpu.VMEM((M, 128), F32),
            pltpu.VMEM((Pn, 128), F32),
            pltpu.VMEM((G, 8, SL), F32),
            pltpu.VMEM((T, 8, Pn), F32),
            pltpu.VMEM((T, KR + 8, M), F32),
            pltpu.VMEM((G, G, 128), F32),
            pltpu.VMEM((G, Fd // 128, 128), F32),
            pltpu.VMEM((G, Fd // 128, 128), F32),
            pltpu.VMEM((G, Fd // 128, 128), F32),
            pltpu.VMEM((8, Fd), F32),
            dma, dma((N,)), dma((nA,)), dma((N,)),
            dma((G,)), dma((G,)), dma((T,)), dma((T,)), dma((T,)), dma((T,)),
            dma((G,)), dma((G,)), dma((G,)), dma((G,)), dma((G,)), dma((G,)),
        ],
        compiler_params=pltpu.CompilerParams(
            collective_id=0, has_side_effects=True, vmem_limit_bytes=60 * 1024 * 1024),
    )(hidden, merge_weight, text_embed, gain[None, :], head_weight.T, owner.T,
      vis_row, lengths, labels, targets)
    reward, grad, head, gg = pl.pallas_call(
        finish,
        name="finish",
        out_shape=(
            jax.ShapeDtypeStruct((1, K), F32),
            jax.ShapeDtypeStruct((M, Fd), BF16),
            jax.ShapeDtypeStruct((K, Fd), F32),
            jax.ShapeDtypeStruct((1, Fd), F32),
        ),
        in_specs=[hbm, vmem, vmem, vmem, vmem, vmem, vmem],
        out_specs=(vmem, hbm, vmem, vmem),
        scratch_shapes=[
            pltpu.VMEM((M, Fd), BF16), pltpu.VMEM((M, Fd), BF16), dma((N,)), dma((N,))],
    )(x, lhs, rhs, bcol, reward, head, gg)
    return reward, grad, head.T, gg[0]


def solution(mesh):
    placed = (
        P("grp", None),
        P(None, "tp"),
        P("grp", "tp"),
        P("tp"),
        P("tp", None),
        P("grp", None),
        P("grp", None),
        P("grp"),
        P(),
        P("grp", None),
    )
    return jax.shard_map(
        on_device,
        mesh=mesh,
        in_specs=placed,
        out_specs=(P("grp", None), P("grp", "tp"), P("tp", None), P("tp")),
        check_vma=False,
    )
```
